32 devices in a mesh: walker: 2 (over x), owner: 4 (over y, core), replica: 4 (over z).
Axes of the slice: x: 2, y: 2, z: 4, core: 2. Of those that a mesh axis runs over, the one named last changes fastest.
Arguments:
- layer_inputs: bfloat16 [4, 61440, 832], P(None, ('walker', 'owner', 'replica')), may hold values from -6 to 6
- layer_grads: bfloat16 [4, 61440, 256], P(None, ('walker', 'owner', 'replica')), may hold values from -6 to 6
- local_energy: float32 [1024], P(('walker', 'owner', 'replica')), may hold values from -3 to 1
Outputs:
- step: float32 [4, 832, 256], replicated
The draws below stay inside these ranges and needn't reach their ends.
All inputs are finite; a program needn't handle non-finite values.
Results may differ from the reference program's by a relative error of at most 0.003.
Values sent between devices are 32-bit elements; how exact they have to be, the bound alone decides.
No kernel may reach another device: no remote copies, remote signals or barrier semaphores. Data moves between devices by JAX's collectives and lax.ppermute only.
A program may use at most 128 MiB of HBM per device.

```python
import jax
import jax.numpy as jnp

HID = 256
ELEC = 60
LAYERS = 4
IN = 832
WALKERS = 1024
ROWS = 61440


def shard_levels(stream_key, shape, pieces, least, top_value):
    loudness, own = 1.0, jax.random.fold_in(stream_key, 6)
    for dim, parts in pieces:
        steps = jnp.exp(jax.random.uniform(jax.random.fold_in(own, dim), (parts,), jnp.float32, least / len(pieces), top_value / len(pieces)))
        loudness = loudness * jnp.repeat(steps, shape[dim] // parts).reshape([-1 if axis == dim else 1 for axis in range(len(shape))])
    return loudness


def centred(stream_key, extent, spread, most, pieces=(), kind=jnp.bfloat16):
    drawn = jax.random.normal(stream_key, extent, jnp.float32) * spread
    if len(pieces) > 0:
        drawn = shard_levels(stream_key, extent, pieces, -0.22, 0.18) * drawn
    return jnp.clip(drawn, min=-most, max=most).astype(kind)


def setup_inputs(seed: int = 0) -> dict:
    keys = jax.random.split(jax.random.key(seed), 4)
    layer_inputs = centred(keys[0], (LAYERS, ROWS, IN), 1.0, 6.0, ((1, 32),))
    layer_grads = centred(keys[1], (LAYERS, ROWS, HID), 1.0, 6.0, ((1, 32),))
    local_energy = jnp.clip(-3.0 + 4.0 * jax.random.uniform(keys[2], (WALKERS,), jnp.float32) ** shard_levels(keys[2], (WALKERS,), ((0, 32),), -0.2, 0.2), -3.0, 1.0)
    return dict(layer_inputs=layer_inputs, layer_grads=layer_grads, local_energy=local_energy)


def reference(layer_inputs, layer_grads, local_energy):
    walkers = local_energy.shape[0]
    rows = layer_inputs.shape[1]
    mean = jnp.sum(local_energy) / walkers
    centered = local_energy - mean
    precs = []
    align = jnp.zeros((), jnp.float32)
    for layer in range(LAYERS):
        inputs = layer_inputs[layer]
        grads = layer_grads[layer]
        weighted = (grads.astype(jnp.float32).reshape(walkers, ELEC, HID) * centered[:, None, None]).astype(jnp.bfloat16).reshape(rows, HID)
        ain = jnp.dot(inputs.T.astype(jnp.float32), inputs.astype(jnp.float32), preferred_element_type=jnp.float32) / rows + 0.1 * jnp.eye(IN, dtype=jnp.float32)
        gout = jnp.dot(grads.T.astype(jnp.float32), grads.astype(jnp.float32), preferred_element_type=jnp.float32) / rows + 0.1 * jnp.eye(HID, dtype=jnp.float32)
        grad = jnp.dot(inputs.T.astype(jnp.float32), weighted.astype(jnp.float32), preferred_element_type=jnp.float32) * (2.0 / walkers)
        chol_in = jnp.linalg.cholesky(ain)
        chol_out = jnp.linalg.cholesky(gout)
        left = jax.scipy.linalg.cho_solve((chol_in, True), grad)
        precond = jax.scipy.linalg.cho_solve((chol_out, True), left.T).T
        align = align + jnp.sum(precond * grad)
        precs.append(precond)
    stacked = jnp.stack(precs, 0)
    return stacked * jnp.sqrt(LAYERS * IN * HID / align)
```

```python
import functools

import jax
import jax.numpy as jnp
from jax import lax
from jax.experimental import pallas as pl
from jax.experimental.pallas import tpu as pltpu
from jax.sharding import PartitionSpec as P

F32 = jnp.float32
BF16 = jnp.bfloat16
LANES = 128
DAMPING = 0.1
TOL = 2e-4
MAX_STEPS = 4000
VMEM = pl.BlockSpec(memory_space=pltpu.VMEM)
SMEM = pl.BlockSpec(memory_space=pltpu.SMEM)
BIG_VMEM = 60 * 1024 * 1024


def gram(a, b):
    return lax.dot_general(a, b, (((0,), (0,)), ((), ())), preferred_element_type=F32)


def layout(width_in, width_out):
    full = width_in // LANES
    blocks = [("a", i, j) for i in range(full) for j in range(i, full)]
    out_blocks = [
        ("g", i, j) for i in range(width_out // LANES) for j in range(i, width_out // LANES)
    ]
    cut = 2 * full - 1
    first = blocks[:cut] + out_blocks
    second = blocks[cut:]
    return first, second


def half_rows(width_in, width_out):
    first, second = layout(width_in, width_out)
    tail = width_in % LANES
    strips = -(-width_in // LANES)
    rows = max(len(first) * LANES, len(second) * LANES + strips * tail)
    return -(-rows // 64) * 64


def factor_kernel(half_ref, x_ref, g_ref, o_ref):
    width_in = x_ref.shape[2]
    width_out = g_ref.shape[2]
    full = width_in // LANES
    tail = width_in % LANES
    first, second = layout(width_in, width_out)
    rows = o_ref.shape[1]

    def panel(i, start):
        lo = i * LANES
        hi = min(i + 2, full) * LANES
        sums = gram(x_ref[0, :, lo:hi], x_ref[0, :, lo : full * LANES])
        at = start
        for b in range((hi - lo) // LANES):
            for j in range(b, full - i):
                o_ref[0, at : at + LANES, :] = sums[
                    b * LANES : (b + 1) * LANES, j * LANES : (j + 1) * LANES
                ]
                at += LANES
        return at

    @pl.when(half_ref[0] == 0)
    def _():
        at = panel(0, 0)
        sums = gram(g_ref[0], g_ref[0])
        for i in range(width_out // LANES):
            for j in range(i, width_out // LANES):
                o_ref[0, at : at + LANES, :] = sums[
                    i * LANES : (i + 1) * LANES, j * LANES : (j + 1) * LANES
                ]
                at += LANES
        if at < rows:
            o_ref[0, at:, :] = jnp.zeros((rows - at, LANES), F32)

    @pl.when(half_ref[0] == 1)
    def _():
        at = 0
        for i in range(2, full, 2):
            at = panel(i, at)
        if tail:
            last = x_ref[0, :, full * LANES :]
            strip = gram(last, x_ref[0, :, : full * LANES])
            for j in range(full):
                o_ref[0, at : at + tail, :] = strip[:, j * LANES : (j + 1) * LANES]
                at += tail
            corner = gram(last, last)
            o_ref[0, at : at + tail, :] = jnp.zeros((tail, LANES), F32)
            o_ref[0, at : at + tail, :tail] = corner
            at += tail
        if at < rows:
            o_ref[0, at:, :] = jnp.zeros((rows - at, LANES), F32)


def factor_sums(half, x, g):
    layers, rows, width_in = x.shape
    width_out = g.shape[2]
    packed = half_rows(width_in, width_out)
    return pl.pallas_call(
        factor_kernel,
        out_shape=jax.ShapeDtypeStruct((layers, packed, LANES), F32),
        grid_spec=pltpu.PrefetchScalarGridSpec(
            num_scalar_prefetch=1,
            grid=(layers,),
            in_specs=[
                pl.BlockSpec((1, rows, width_in), lambda l, s: (l, 0, 0)),
                pl.BlockSpec((1, rows, width_out), lambda l, s: (l, 0, 0)),
            ],
            out_specs=pl.BlockSpec((1, packed, LANES), lambda l, s: (l, 0, 0)),
        ),
        compiler_params=pltpu.CompilerParams(vmem_limit_bytes=BIG_VMEM),
        cost_estimate=pl.CostEstimate(
            flops=layers * rows * width_in * width_in,
            bytes_accessed=layers * (rows * (width_in + width_out) * 2 + packed * LANES * 4),
            transcendentals=0,
        ),
        name="factor_sums",
    )(half, x, g)


def grad_kernel(core_ref, x_ref, g_ref, c_ref, keep_ref, send_ref):
    parts = [
        (g_ref[0, :, j : j + LANES].astype(F32) * c_ref[...]).astype(BF16)
        for j in range(0, g_ref.shape[2], LANES)
    ]
    sums = gram(x_ref[0], jnp.concatenate(parts, axis=1))

    @pl.when(core_ref[0] == 0)
    def _():
        keep_ref[0] = sums[:, :LANES]
        send_ref[0] = sums[:, LANES:]

    @pl.when(core_ref[0] == 1)
    def _():
        keep_ref[0] = sums[:, LANES:]
        send_ref[0] = sums[:, :LANES]


def grad_sums(core, x, g, centered):
    layers, rows, width_in = x.shape
    width_out = g.shape[2]
    out = jax.ShapeDtypeStruct((layers, width_in, LANES), F32)
    out_spec = pl.BlockSpec((1, width_in, LANES), lambda l, s: (l, 0, 0))
    return pl.pallas_call(
        grad_kernel,
        out_shape=(out, out),
        grid_spec=pltpu.PrefetchScalarGridSpec(
            num_scalar_prefetch=1,
            grid=(layers,),
            in_specs=[
                pl.BlockSpec((1, rows, width_in), lambda l, s: (l, 0, 0)),
                pl.BlockSpec((1, rows, width_out), lambda l, s: (l, 0, 0)),
                pl.BlockSpec((rows, LANES), lambda l, s: (0, 0)),
            ],
            out_specs=(out_spec, out_spec),
        ),
        compiler_params=pltpu.CompilerParams(vmem_limit_bytes=BIG_VMEM),
        cost_estimate=pl.CostEstimate(
            flops=2 * layers * rows * width_in * width_out,
            bytes_accessed=layers * (rows * (width_in + width_out) * 2 + width_in * width_out * 4),
            transcendentals=0,
        ),
        name="grad_sums",
    )(core, x, g, centered)


def split3(v):
    one = v.astype(BF16)
    rest = v - one.astype(F32)
    two = rest.astype(BF16)
    three = (rest - two.astype(F32)).astype(BF16)
    return one, two, three


def mm(a, b):
    return jnp.dot(a, b, preferred_element_type=F32)


def product(a, b):
    low = mm(a[0], b[2]) + mm(a[2], b[0]) + mm(a[1], b[1])
    return mm(a[0], b[0]) + (mm(a[0], b[1]) + mm(a[1], b[0]) + low)


def conjugate_gradients(apply, y_ref, r_ref, p_ref):
    r = r_ref[...]
    p_ref[...] = r
    y_ref[...] = jnp.zeros_like(r)

    def go_on(state):
        step, residual, size = state
        return (residual > (TOL * DAMPING) ** 2 * size) & (step < MAX_STEPS)

    def body(state):
        step, residual, _ = state
        q = apply(p_ref[...])
        alpha = residual / jnp.sum(p_ref[...] * q)
        y = y_ref[...] + alpha * p_ref[...]
        y_ref[...] = y
        r = r_ref[...] - alpha * q
        r_ref[...] = r
        fresh = jnp.sum(r * r)
        p_ref[...] = r + (fresh / residual) * p_ref[...]
        return step + 1, fresh, jnp.sum(y * y)

    lax.while_loop(go_on, body, (jnp.int32(0), jnp.sum(r * r), jnp.float32(0.0)))


def solve_kernel(
    all_rows,
    walkers,
    width_in,
    width_out,
    s_ref,
    own0,
    own1,
    own2,
    got0,
    got1,
    got2,
    mine_ref,
    other_ref,
    a0,
    a1,
    a2,
    g0,
    g1,
    g2,
    b_ref,
    y_ref,
    r_ref,
    p_ref,
):
    full = width_in // LANES
    tail = width_in % LANES
    first, second = layout(width_in, width_out)
    terms = {"a": (a0, a1, a2), "g": (g0, g1, g2)}

    def put(kind, row, col, value):
        height, width = value.shape
        for ref, term in zip(terms[kind], split3(value)):
            ref[row : row + height, col : col + width] = term

    def place(kind, i, j, value):
        value = value * (1.0 / all_rows)
        if i == j:
            rows = lax.broadcasted_iota(jnp.int32, value.shape, 0)
            cols = lax.broadcasted_iota(jnp.int32, value.shape, 1)
            value = value + jnp.where(rows == cols, jnp.float32(DAMPING), 0.0)
        put(kind, i * LANES, j * LANES, value)
        if i != j:
            put(kind, j * LANES, i * LANES, value.T)

    def unpack(half, refs):
        rows = refs[0].shape[0]

        def read(at, height):
            return refs[at // rows][at % rows : at % rows + height, :]

        at = 0
        for kind, i, j in (first, second)[half]:
            place(kind, i, j, read(at, LANES))
            at += LANES
        if half == 1 and tail:
            edge = full * LANES
            for j in range(full):
                value = read(at, tail) * (1.0 / all_rows)
                put("a", edge, j * LANES, value)
                put("a", j * LANES, edge, jnp.concatenate([value, jnp.zeros_like(value)], 0).T[:, :tail])
                at += tail
            value = read(at, tail)[:, :tail] * (1.0 / all_rows)
            rows_at = lax.broadcasted_iota(jnp.int32, value.shape, 0)
            cols_at = lax.broadcasted_iota(jnp.int32, value.shape, 1)
            put("a", edge, edge, value + jnp.where(rows_at == cols_at, jnp.float32(DAMPING), 0.0))
        b_ref[:width_in, half * LANES : (half + 1) * LANES] = refs[2][...] * (2.0 / walkers)

    padded = a0.shape[0]
    if padded > width_in:
        for ref in terms["a"]:
            ref[width_in:, :] = jnp.zeros((padded - width_in, padded), BF16)
            ref[:, width_in:] = jnp.zeros((padded, padded - width_in), BF16)
        b_ref[width_in:, :] = jnp.zeros((padded - width_in, width_out), F32)
    core = s_ref[0]

    @pl.when(core == 0)
    def _():
        unpack(0, (own0, own1, own2))
        unpack(1, (got0, got1, got2))

    @pl.when(core == 1)
    def _():
        unpack(1, (own0, own1, own2))
        unpack(0, (got0, got1, got2))

    r_ref[...] = b_ref[...]
    conjugate_gradients(
        lambda p: product((a0[...], a1[...], a2[...]), split3(p)), y_ref, r_ref, p_ref
    )
    r_ref[...] = y_ref[...]
    conjugate_gradients(
        lambda p: product(split3(p), (g0[...], g1[...], g2[...])), y_ref, r_ref, p_ref
    )
    align = jnp.sum(y_ref[...] * b_ref[...])
    strip = mine_ref.shape[1] - 8

    def give(mine, other):
        for half in range(2):
            mine_ref[half, :strip, :] = mine[half * strip : (half + 1) * strip, :]
            mine_ref[half, strip:, :] = jnp.zeros((8, LANES), F32) + align
        other_ref[...] = other

    @pl.when(core == 0)
    def _():
        give(y_ref[:width_in, :LANES], y_ref[:width_in, LANES:])

    @pl.when(core == 1)
    def _():
        give(y_ref[:width_in, LANES:], y_ref[:width_in, :LANES])


def solve(scalars, own, got, all_rows, walkers, width_in, width_out):
    padded = -(-width_in // LANES) * LANES
    square = pltpu.VMEM((padded, padded), BF16)
    small = pltpu.VMEM((width_out, width_out), BF16)
    tall = pltpu.VMEM((padded, width_out), F32)
    return pl.pallas_call(
        functools.partial(solve_kernel, all_rows, walkers, width_in, width_out),
        out_shape=(
            jax.ShapeDtypeStruct((2, width_in // 2 + 8, LANES), F32),
            jax.ShapeDtypeStruct((width_in, LANES), F32),
        ),
        in_specs=[SMEM] + [VMEM] * 6,
        out_specs=(VMEM, VMEM),
        scratch_shapes=[square] * 3 + [small] * 3 + [tall] * 4,
        compiler_params=pltpu.CompilerParams(vmem_limit_bytes=BIG_VMEM),
        cost_estimate=pl.CostEstimate(
            flops=60 * width_in * width_in * width_out, bytes_accessed=4 << 20, transcendentals=0
        ),
        name="solve",
    )(scalars, *own, *got)


def finish_kernel(count, s_ref, mine, other, a1, a2, b1, b2, ca1, ca2, cb1, cb2, out_ref):
    core = s_ref[0]
    layer = s_ref[1]
    strip = mine.shape[1] - 8
    top = {0: mine[0], 2: a1[...], 1: a2[0], 3: a2[1]}
    low = {0: mine[1], 1: b1[...], 2: b2[0], 3: b2[1]}
    far_top = {2: ca1[...], 1: ca2[0], 3: ca2[1]}
    far_low = {1: cb1[...], 2: cb2[0], 3: cb2[1]}
    a = [top[k][strip : strip + 1, :] for k in range(4)]
    align = (a[0] + a[1]) + (a[2] + a[3])
    scale = jnp.sqrt(count / align)
    here = pl.ds(pl.multiple_of(core * LANES, LANES), LANES)
    there = pl.ds(pl.multiple_of((1 - core) * LANES, LANES), LANES)
    for k in range(4):
        at = layer ^ k
        out_ref[at, :strip, here] = top[k][:strip, :] * scale
        out_ref[at, strip:, here] = low[k][:strip, :] * scale
        if k:
            out_ref[at, :strip, there] = far_top[k][:strip, :] * scale
            out_ref[at, strip:, there] = far_low[k][:strip, :] * scale
        else:
            out_ref[at, :, there] = other[...] * scale


def finish(scalars, pieces, layers, width_in, width_out):
    return pl.pallas_call(
        functools.partial(finish_kernel, float(layers * width_in * width_out)),
        out_shape=jax.ShapeDtypeStruct((layers, width_in, width_out), F32),
        in_specs=[SMEM] + [VMEM] * len(pieces),
        out_specs=VMEM,
        compiler_params=pltpu.CompilerParams(vmem_limit_bytes=BIG_VMEM),
        name="finish",
    )(scalars, *pieces)


def swap(value, axis, bit):
    size = lax.axis_size(axis)
    return lax.ppermute(value, axis, [(i, i ^ bit) for i in range(size)])


def bit_of(axis, bit):
    return (lax.axis_index(axis) // bit) % 2


def pick(value, dim, index):
    return lax.dynamic_index_in_dim(value, index, dim, keepdims=False)


def shards(layer_inputs, layer_grads, local_energy):
    walk_count = lax.axis_size("walker")
    devices = walk_count * lax.axis_size("owner") * lax.axis_size("replica")
    per_walker = local_energy.shape[0]
    walkers = per_walker * devices
    layers, rows, width_in = layer_inputs.shape
    width_out = layer_grads.shape[2]
    all_rows = rows * devices

    core_bit = ("owner", 1)
    first_bit = ("walker", 1)
    second_bit = ("replica", 1)
    row_bits = [("owner", 2), ("replica", 2)]
    extra = 2
    while extra < walk_count:
        row_bits.append(("walker", extra))
        extra *= 2

    core = bit_of(*core_bit).astype(jnp.int32)
    bx = bit_of(*first_bit)
    bd = bit_of(*second_bit)
    layer = (2 * bx + bd).astype(jnp.int32)

    total = jnp.broadcast_to(jnp.sum(local_energy), (8, LANES))
    for axis in ("replica", "owner", "walker"):
        size = lax.axis_size(axis)
        total = total + sum(
            lax.ppermute(total, axis, [(i, (i + k) % size) for i in range(size)])
            for k in range(1, size)
        )
    centered = local_energy[:, None] - total[:1, :] / walkers
    centered = jnp.repeat(centered, rows // per_walker, axis=0)

    send = factor_sums((1 - core).reshape(1), layer_inputs, layer_grads)
    got_factors = swap(send, *core_bit)
    keep_factors = factor_sums(core.reshape(1), layer_inputs, layer_grads)
    keep_grads, send_grads = grad_sums(core.reshape(1), layer_inputs, layer_grads, centered)
    got_grads = swap(send_grads, *core_bit)

    packed = keep_factors.shape[1] // 2
    colours = [
        (keep_factors[:, :packed], got_factors[:, :packed]),
        (keep_factors[:, packed:], got_factors[:, packed:]),
        (keep_grads, got_grads),
    ]
    orders = [
        [0, 2, 1],
        [2, 1, 0],
        [1, 0, 2],
    ]
    bits = [first_bit, second_bit] + row_bits
    sums = []
    for (keep, got), order in zip(colours, orders):
        order = order + list(range(3, len(bits)))
        shape = (2, 2) + (2,) * len(row_bits) + (-1, LANES)
        keep = keep.reshape(shape)
        got = got.reshape(shape)
        left = list(range(len(bits)))
        for which in order:
            dim = left.index(which)
            mine = bit_of(*bits[which])
            out = pick(keep, dim, 1 - mine) + pick(got, dim, 1 - mine)
            stay = pick(keep, dim, mine) + pick(got, dim, mine)
            got = swap(out, *bits[which])
            keep = stay
            left.remove(which)
        piece = keep + got
        back = [w for w in order if w >= 2][::-1]
        dims = []
        for which in back:
            mine = bit_of(*bits[which])
            other = swap(piece, *bits[which])
            low = jnp.where(mine == 0, piece, other)
            high = jnp.where(mine == 0, other, piece)
            piece = jnp.stack([low, high])
            dims.insert(0, which)
        rank = len(dims)
        axes = sorted(range(rank), key=lambda k: dims[k])
        piece = piece.transpose(*axes, rank, rank + 1).reshape(-1, LANES)
        sums.append(piece)

    got = [swap(piece, *core_bit) for piece in sums]
    scalars = jnp.stack([core, layer])
    mine, other = solve(scalars, sums, got, all_rows, walkers, width_in, width_out)

    a1 = swap(mine[0], *first_bit)
    b1 = swap(mine[1], *second_bit)
    ca1 = swap(a1, *core_bit)
    cb1 = swap(b1, *core_bit)
    a2 = swap(jnp.stack([mine[0], a1]), *second_bit)
    b2 = swap(jnp.stack([mine[1], b1]), *first_bit)
    ca2 = swap(a2, *core_bit)
    cb2 = swap(b2, *core_bit)
    return finish(
        scalars,
        (mine, other, a1, a2, b1, b2, ca1, ca2, cb1, cb2),
        layers,
        width_in,
        width_out,
    )


def solution(mesh):
    in_specs = (
        P(None, ("walker", "owner", "replica"), None),
        P(None, ("walker", "owner", "replica"), None),
        P(("walker", "owner", "replica")),
    )
    return jax.shard_map(shards, mesh=mesh, in_specs=in_specs, out_specs=P(), check_vma=False)
```

```python
import functools

import jax
import jax.numpy as jnp
from jax import lax
from jax.experimental import pallas as pl
from jax.experimental.pallas import tpu as pltpu
from jax.sharding import PartitionSpec as P


F32 = jnp.float32
BF16 = jnp.bfloat16
LANES = 128
DAMPING = 0.1
TOL = 5e-4
MAX_STEPS = 4000
VMEM = pl.BlockSpec(memory_space=pltpu.VMEM)
SMEM = pl.BlockSpec(memory_space=pltpu.SMEM)
BIG_VMEM = 60 * 1024 * 1024


def gram(a, b):
    return lax.dot_general(a, b, (((0,), (0,)), ((), ())), preferred_element_type=F32)


def outer(a, b):
    return lax.dot_general(a, b, (((1,), (1,)), ((), ())), preferred_element_type=F32)


def layout(width_in, width_out):
    full = width_in // LANES
    blocks = [("a", i, j) for i in range(full) for j in range(i, full)]
    out_blocks = [
        ("g", i, j) for i in range(width_out // LANES) for j in range(i, width_out // LANES)
    ]
    cut = 2 * full - 1
    first = blocks[:cut] + out_blocks
    second = blocks[cut:]
    return first, second


def half_rows(width_in, width_out):
    first, second = layout(width_in, width_out)
    tail = width_in % LANES
    strips = -(-width_in // LANES)
    rows = max(len(first) * LANES, len(second) * LANES + strips * tail)
    return -(-rows // 64) * 64


def factor_kernel(where_ref, x_ref, g_ref, keep_ref, send_ref):
    width_in = x_ref.shape[1]
    width_out = g_ref.shape[2]
    full = width_in // LANES
    tail = width_in % LANES
    rows = keep_ref.shape[1]

    def panel(o_ref, i, start):
        lo = i * LANES
        hi = min(i + 2, full) * LANES
        sums = outer(x_ref[0, lo : full * LANES, :], x_ref[0, lo:hi, :])
        at = start
        for b in range((hi - lo) // LANES):
            for j in range(b, full - i):
                o_ref[0, at : at + LANES, :] = sums[
                    j * LANES : (j + 1) * LANES, b * LANES : (b + 1) * LANES
                ]
                at += LANES
        return at

    def first_half(o_ref):
        at = panel(o_ref, 0, 0)
        sums = gram(g_ref[0], g_ref[0])
        for i in range(width_out // LANES):
            for j in range(i, width_out // LANES):
                o_ref[0, at : at + LANES, :] = sums[
                    j * LANES : (j + 1) * LANES, i * LANES : (i + 1) * LANES
                ]
                at += LANES
        if at < rows:
            o_ref[0, at:, :] = jnp.zeros((rows - at, LANES), F32)

    def second_half(o_ref):
        at = 0
        for i in range(2, full, 2):
            at = panel(o_ref, i, at)
        if tail:
            last = x_ref[0, full * LANES :, :]
            strip = outer(last, x_ref[0, : full * LANES, :])
            for j in range(full):
                o_ref[0, at : at + tail, :] = strip[:, j * LANES : (j + 1) * LANES]
                at += tail
            corner = outer(last, last)
            o_ref[0, at : at + tail, :] = jnp.zeros((tail, LANES), F32)
            o_ref[0, at : at + tail, :tail] = corner
            at += tail
        if at < rows:
            o_ref[0, at:, :] = jnp.zeros((rows - at, LANES), F32)

    @pl.when(where_ref[0] == 0)
    def _():
        first_half(keep_ref)
        second_half(send_ref)

    @pl.when(where_ref[0] == 1)
    def _():
        first_half(send_ref)
        second_half(keep_ref)


def factor_sums(where, first, layers, x, g):
    _, width_in, rows = x.shape
    width_out = g.shape[2]
    packed = half_rows(width_in, width_out)
    out = jax.ShapeDtypeStruct((layers, packed, LANES), F32)
    out_spec = pl.BlockSpec((1, packed, LANES), lambda l, s: (l, 0, 0))
    return pl.pallas_call(
        factor_kernel,
        out_shape=(out, out),
        grid_spec=pltpu.PrefetchScalarGridSpec(
            num_scalar_prefetch=1,
            grid=(layers,),
            in_specs=[
                pl.BlockSpec((1, width_in, rows), lambda l, s: ((l + first) ^ s[1], 0, 0)),
                pl.BlockSpec((1, rows, width_out), lambda l, s: ((l + first) ^ s[1], 0, 0)),
            ],
            out_specs=(out_spec, out_spec),
        ),
        compiler_params=pltpu.CompilerParams(vmem_limit_bytes=BIG_VMEM),
        cost_estimate=pl.CostEstimate(
            flops=layers * rows * width_in * width_in,
            bytes_accessed=layers * (rows * (width_in + width_out) * 2 + packed * LANES * 8),
            transcendentals=0,
        ),
        name="factor_sums",
    )(where, x, g)


def grad_kernel(core_ref, x_ref, g_ref, c_ref, keep_ref, send_ref):
    parts = [
        (g_ref[0, :, j : j + LANES].astype(F32) * c_ref[...]).astype(BF16)
        for j in range(0, g_ref.shape[2], LANES)
    ]
    sums = mm(x_ref[0], jnp.concatenate(parts, axis=1))

    @pl.when(core_ref[0] == 0)
    def _():
        keep_ref[0] = sums[:, :LANES]
        send_ref[0] = sums[:, LANES:]

    @pl.when(core_ref[0] == 1)
    def _():
        keep_ref[0] = sums[:, LANES:]
        send_ref[0] = sums[:, :LANES]


def grad_sums(where, x, g, centered):
    layers, width_in, rows = x.shape
    width_out = g.shape[2]
    out = jax.ShapeDtypeStruct((layers, width_in, LANES), F32)
    out_spec = pl.BlockSpec((1, width_in, LANES), lambda l, s: (l, 0, 0))
    return pl.pallas_call(
        grad_kernel,
        out_shape=(out, out),
        grid_spec=pltpu.PrefetchScalarGridSpec(
            num_scalar_prefetch=1,
            grid=(layers,),
            in_specs=[
                pl.BlockSpec((1, width_in, rows), lambda l, s: (l ^ s[1], 0, 0)),
                pl.BlockSpec((1, rows, width_out), lambda l, s: (l ^ s[1], 0, 0)),
                pl.BlockSpec((rows, LANES), lambda l, s: (0, 0)),
            ],
            out_specs=(out_spec, out_spec),
        ),
        compiler_params=pltpu.CompilerParams(vmem_limit_bytes=BIG_VMEM),
        cost_estimate=pl.CostEstimate(
            flops=2 * layers * rows * width_in * width_out,
            bytes_accessed=layers * (rows * (width_in + width_out) * 2 + width_in * width_out * 4),
            transcendentals=0,
        ),
        name="grad_sums",
    )(where, x, g, centered)


def split3(v):
    one = v.astype(BF16)
    rest = v - one.astype(F32)
    two = rest.astype(BF16)
    three = (rest - two.astype(F32)).astype(BF16)
    return one, two, three


def mm(a, b):
    return jnp.dot(a, b, preferred_element_type=F32)


def product(a, b):
    low = mm(a[0], b[2]) + mm(a[2], b[0]) + mm(a[1], b[1])
    return mm(a[0], b[0]) + (mm(a[0], b[1]) + mm(a[1], b[0]) + low)


def conjugate_gradients(apply, exact, b_ref, y_ref, r_ref, p_ref):
    def total(v):
        return jnp.sum(v, keepdims=True)

    def wanted(residual, size):
        return (residual - (TOL * DAMPING) ** 2 * size)[0, 0] > 0

    def body(state):
        step, residual, _ = state
        p = p_ref[...]
        q = apply(p)
        alpha = residual / total(p * q)
        y = y_ref[...] + alpha * p
        y_ref[...] = y
        r = r_ref[...] - alpha * q
        r_ref[...] = r
        fresh = total(r * r)
        p_ref[...] = r + (fresh / residual) * p
        return step + 1, fresh, wanted(fresh, total(y * y))

    def steps(start):
        r = r_ref[...]
        p_ref[...] = r
        residual = total(r * r)
        step, _, _ = lax.while_loop(
            lambda state: state[2] & (state[0] < MAX_STEPS),
            body,
            (start, residual, residual[0, 0] > 0),
        )
        return step

    y_ref[...] = jnp.zeros(y_ref.shape, F32)
    r_ref[...] = b_ref[...]
    if exact is None:
        steps(jnp.int32(0))
        return

    def cycle(state):
        step = steps(state[0])
        y = y_ref[...]
        r = b_ref[...] - exact(y)
        r_ref[...] = r
        return step, wanted(total(r * r), total(y * y))

    lax.while_loop(
        lambda state: state[1] & (state[0] < MAX_STEPS), cycle, (jnp.int32(0), jnp.bool_(True))
    )


def solve_kernel(
    all_rows,
    walkers,
    width_in,
    width_out,
    s_ref,
    own0,
    own1,
    own2,
    got0,
    got1,
    got2,
    mine_ref,
    other_ref,
    a0,
    a1,
    a2,
    g0,
    g1,
    g2,
    b_ref,
    t_ref,
    y_ref,
    r_ref,
    p_ref,
):
    full = width_in // LANES
    tail = width_in % LANES
    first, second = layout(width_in, width_out)
    terms = {"a": (a0, a1, a2), "g": (g0, g1, g2)}

    def put(kind, row, col, value):
        height, width = value.shape
        for ref, term in zip(terms[kind], split3(value)):
            ref[row : row + height, col : col + width] = term

    def place(kind, i, j, value):
        value = value * (1.0 / all_rows)
        if i == j:
            rows = lax.broadcasted_iota(jnp.int32, value.shape, 0)
            cols = lax.broadcasted_iota(jnp.int32, value.shape, 1)
            value = value + jnp.where(rows == cols, jnp.float32(DAMPING), 0.0)
        put(kind, j * LANES, i * LANES, value)
        if i != j:
            put(kind, i * LANES, j * LANES, value.T)

    def unpack(half, refs):
        rows = refs[0].shape[0]

        def read(at, height):
            return refs[at // rows][at % rows : at % rows + height, :]

        at = 0
        for kind, i, j in (first, second)[half]:
            place(kind, i, j, read(at, LANES))
            at += LANES
        if half == 1 and tail:
            edge = full * LANES
            for j in range(full):
                value = read(at, tail) * (1.0 / all_rows)
                put("a", edge, j * LANES, value)
                put("a", j * LANES, edge, jnp.concatenate([value, jnp.zeros_like(value)], 0).T[:, :tail])
                at += tail
            value = read(at, tail)[:, :tail] * (1.0 / all_rows)
            rows_at = lax.broadcasted_iota(jnp.int32, value.shape, 0)
            cols_at = lax.broadcasted_iota(jnp.int32, value.shape, 1)
            put("a", edge, edge, value + jnp.where(rows_at == cols_at, jnp.float32(DAMPING), 0.0))
        b_ref[:width_in, half * LANES : (half + 1) * LANES] = refs[2][...] * (2.0 / walkers)

    padded = a0.shape[0]
    if padded > width_in:
        for ref in terms["a"]:
            ref[width_in:, :] = jnp.zeros((padded - width_in, padded), BF16)
            ref[:, width_in:] = jnp.zeros((padded, padded - width_in), BF16)
        b_ref[width_in:, :] = jnp.zeros((padded - width_in, width_out), F32)
    core = s_ref[0]

    @pl.when(core == 0)
    def _():
        unpack(0, (own0, own1, own2))
        unpack(1, (got0, got1, got2))

    @pl.when(core == 1)
    def _():
        unpack(1, (own0, own1, own2))
        unpack(0, (got0, got1, got2))

    def near(p):
        one = p.astype(BF16)
        two = (p - one.astype(F32)).astype(BF16)
        return mm(a0[...], one) + (mm(a0[...], two) + mm(a1[...], one))

    conjugate_gradients(
        near,
        lambda p: product((a0[...], a1[...], a2[...]), split3(p)),
        b_ref,
        t_ref,
        r_ref,
        p_ref,
    )
    conjugate_gradients(
        lambda p: product(split3(p), (g0[...], g1[...], g2[...])), None, t_ref, y_ref, r_ref, p_ref
    )
    align = jnp.sum(y_ref[...] * b_ref[...])
    strip = mine_ref.shape[1] - 8

    def give(mine, other):
        for half in range(2):
            mine_ref[half, :strip, :] = mine[half * strip : (half + 1) * strip, :]
            mine_ref[half, strip:, :] = jnp.zeros((8, LANES), F32) + align
        other_ref[...] = other

    @pl.when(core == 0)
    def _():
        give(y_ref[:width_in, :LANES], y_ref[:width_in, LANES:])

    @pl.when(core == 1)
    def _():
        give(y_ref[:width_in, LANES:], y_ref[:width_in, :LANES])


def solve(scalars, own, got, all_rows, walkers, width_in, width_out):
    padded = -(-width_in // LANES) * LANES
    square = pltpu.VMEM((padded, padded), BF16)
    small = pltpu.VMEM((width_out, width_out), BF16)
    tall = pltpu.VMEM((padded, width_out), F32)
    return pl.pallas_call(
        functools.partial(solve_kernel, all_rows, walkers, width_in, width_out),
        out_shape=(
            jax.ShapeDtypeStruct((2, width_in // 2 + 8, LANES), F32),
            jax.ShapeDtypeStruct((width_in, LANES), F32),
        ),
        in_specs=[SMEM] + [VMEM] * 6,
        out_specs=(VMEM, VMEM),
        scratch_shapes=[square] * 3 + [small] * 3 + [tall] * 5,
        compiler_params=pltpu.CompilerParams(vmem_limit_bytes=BIG_VMEM),
        cost_estimate=pl.CostEstimate(
            flops=60 * width_in * width_in * width_out, bytes_accessed=4 << 20, transcendentals=0
        ),
        name="solve",
    )(scalars, *own, *got)


def finish_kernel(count, s_ref, mine, other, *refs):
    near, far, out_ref = refs[:6], refs[6:12], refs[12]
    core = s_ref[0]
    layer = s_ref[1]
    strip = mine.shape[1] - 8
    top = {0: mine[0], **{k: near[k - 1][...] for k in (1, 2, 3)}}
    low = {0: mine[1], **{k: near[k + 2][...] for k in (1, 2, 3)}}
    a = [top[k][strip : strip + 1, :] for k in range(4)]
    align = (a[0] + a[1]) + (a[2] + a[3])
    scale = jnp.sqrt(count / align)
    here = pl.ds(pl.multiple_of(core * LANES, LANES), LANES)
    there = pl.ds(pl.multiple_of((1 - core) * LANES, LANES), LANES)
    for k in range(4):
        at = layer ^ k
        out_ref[at, :strip, here] = top[k][:strip, :] * scale
        out_ref[at, strip:, here] = low[k][:strip, :] * scale
        if k:
            out_ref[at, :strip, there] = far[k - 1][:strip, :] * scale
            out_ref[at, strip:, there] = far[k + 2][:strip, :] * scale
        else:
            out_ref[at, :, there] = other[...] * scale


def finish(scalars, pieces, layers, width_in, width_out):
    return pl.pallas_call(
        functools.partial(finish_kernel, float(layers * width_in * width_out)),
        out_shape=jax.ShapeDtypeStruct((layers, width_in, width_out), F32),
        in_specs=[SMEM] + [VMEM] * len(pieces),
        out_specs=VMEM,
        compiler_params=pltpu.CompilerParams(vmem_limit_bytes=BIG_VMEM),
        name="finish",
    )(scalars, *pieces)


def swap(value, axis, bit):
    size = lax.axis_size(axis)
    return lax.ppermute(value, axis, [(i, i ^ bit) for i in range(size)])


def bit_of(axis, bit):
    return (lax.axis_index(axis) // bit) % 2


def pick(value, dim, index):
    return lax.dynamic_index_in_dim(value, index, dim, keepdims=False)


def shard_step(layer_inputs, layer_grads, local_energy):
    walk_count = lax.axis_size("walker")
    devices = walk_count * lax.axis_size("owner") * lax.axis_size("replica")
    per_walker = local_energy.shape[0]
    walkers = per_walker * devices
    layers, rows, width_in = layer_inputs.shape
    width_out = layer_grads.shape[2]
    all_rows = rows * devices

    core_bit = ("owner", 1)
    first_bit = ("walker", 1)
    second_bit = ("replica", 1)
    row_bits = [("owner", 2), ("replica", 2)]
    extra = 2
    while extra < walk_count:
        row_bits.append(("walker", extra))
        extra *= 2

    core = bit_of(*core_bit).astype(jnp.int32)
    bx = bit_of(*first_bit)
    bd = bit_of(*second_bit)
    layer = (2 * bx + bd).astype(jnp.int32)

    inputs = jnp.swapaxes(layer_inputs, 1, 2)
    scalars = jnp.stack([core, layer])
    tie = lax.optimization_barrier
    half = layers // 2

    total = jnp.broadcast_to(jnp.sum(local_energy), (8, LANES))

    def along(axes, value):
        size = 1
        for axis in axes:
            size *= lax.axis_size(axis)
        return [
            lax.ppermute(value, axes, [(i, (i + k) % size) for i in range(size)])
            for k in range(1, size)
        ]

    terms = along(("replica",), total)
    keep_far, send_far = factor_sums(scalars, half, half, inputs, layer_grads)
    keep_far, send_far, total, terms, where = tie((keep_far, send_far, total, terms, scalars))
    got_far = swap(send_far, *core_bit)
    total = total + sum(terms)
    terms = along(("owner",), total)
    where, total = tie((where, total))
    keep_own, send_own = factor_sums(where, 0, half, inputs, layer_grads)
    keep_own, send_own, total, terms, where = tie((keep_own, send_own, total, terms, where))
    got_own = swap(send_own, *core_bit)
    total = total + sum(terms)
    total = total + sum(along(("walker",), total))
    centered = local_energy[:, None] - total[:1, :] / walkers
    centered = jnp.repeat(centered, rows // per_walker, axis=0)

    bits = [first_bit, second_bit] + row_bits
    inner = (2,) * len(row_bits) + (-1, LANES)
    packed = keep_far.shape[1] // 2

    def start(parts, order):
        which = order[0]
        parts = [[v.reshape((2,) + inner) for v in pair] for pair in parts]
        if which == 0:
            return sum(parts[1]), sum(parts[0])
        if which == 1:
            return tuple(jnp.stack([sum(v[i] for v in pair) for pair in parts]) for i in (1, 0))
        mine = bit_of(*bits[which])
        return tuple(
            jnp.stack([sum(pick(v, which - 1, i) for v in pair) for pair in parts])
            for i in (1 - mine, mine)
        )

    rest = list(range(3, len(bits)))
    orders = [[0, 1, 2] + rest, [1, 0, 2] + rest, [2, 1, 0] + rest]
    out = keep_far[:, :packed] + got_far[:, :packed]
    out, where, centered = tie((out, where, centered))
    out_first = out.reshape((2,) + inner)
    keep_grads, send_grads = grad_sums(where, inputs, layer_grads, centered)
    got_grads = swap(send_grads, *core_bit)
    stay_first = (keep_own[:, :packed] + got_own[:, :packed]).reshape((2,) + inner)
    out_second, stay_second = start(
        [
            [keep_own[:, packed:], got_own[:, packed:]],
            [keep_far[:, packed:], got_far[:, packed:]],
        ],
        orders[1],
    )
    third = start(
        [[keep_grads[:half], got_grads[:half]], [keep_grads[half:], got_grads[half:]]], orders[2]
    )

    sums = []
    for colour, ((out, keep), order) in enumerate(
        zip([(out_first, stay_first), (out_second, stay_second), third], orders)
    ):
        got = swap(out, *bits[order[0]])
        left = list(range(len(bits)))
        left.remove(order[0])
        for which in order[1:]:
            dim = left.index(which)
            if which < 2:
                out = lax.index_in_dim(keep, 1, dim, False) + lax.index_in_dim(got, 1, dim, False)
                stay = lax.index_in_dim(keep, 0, dim, False) + lax.index_in_dim(got, 0, dim, False)
            else:
                mine = bit_of(*bits[which])
                out = pick(keep, dim, 1 - mine) + pick(got, dim, 1 - mine)
                stay = pick(keep, dim, mine) + pick(got, dim, mine)
            got = swap(out, *bits[which])
            keep = stay
            left.remove(which)
        piece = keep + got
        back = [w for w in order if w >= 2]
        if colour < 2:
            back = back[::-1]
        dims = []
        for which in back:
            mine = bit_of(*bits[which])
            other = swap(piece, *bits[which])
            low = jnp.where(mine == 0, piece, other)
            high = jnp.where(mine == 0, other, piece)
            piece = jnp.stack([low, high])
            dims.insert(0, which)
        rank = len(dims)
        axes = sorted(range(rank), key=lambda k: dims[k])
        piece = piece.transpose(*axes, rank, rank + 1).reshape(-1, LANES)
        sums.append(piece)

    got = [swap(piece, *core_bit) for piece in sums]
    mine, other = solve(scalars, sums, got, all_rows, walkers, width_in, width_out)

    top = {2: swap(mine[0], *first_bit), 1: swap(mine[0], *second_bit)}
    low = {1: swap(mine[1], *second_bit), 2: swap(mine[1], *first_bit)}
    top[3] = swap(top[2], *second_bit)
    low[3] = swap(low[1], *first_bit)
    near = [top[k] for k in (1, 2, 3)] + [low[k] for k in (1, 2, 3)]
    far = [swap(piece, *core_bit) for piece in near]
    return finish(scalars, (mine, other, *near, *far), layers, width_in, width_out)


def solution(mesh):
    in_specs = (
        P(None, ("walker", "owner", "replica"), None),
        P(None, ("walker", "owner", "replica"), None),
        P(("walker", "owner", "replica")),
    )
    return jax.shard_map(shard_step, mesh=mesh, in_specs=in_specs, out_specs=P(), check_vma=False)
```

```python
import functools

import jax
import jax.numpy as jnp
from jax import lax
from jax.experimental import pallas as pl
from jax.experimental.pallas import tpu as pltpu
from jax.sharding import PartitionSpec as P


F32 = jnp.float32
BF16 = jnp.bfloat16
LANES = 128
DAMPING = 0.1
TOL = 5e-4
MAX_STEPS = 4000
VMEM = pl.BlockSpec(memory_space=pltpu.VMEM)
SMEM = pl.BlockSpec(memory_space=pltpu.SMEM)
BIG_VMEM = 60 * 1024 * 1024


def gram(a, b):
    return lax.dot_general(a, b, (((0,), (0,)), ((), ())), preferred_element_type=F32)


def outer(a, b):
    return lax.dot_general(a, b, (((1,), (1,)), ((), ())), preferred_element_type=F32)


def layout(width_in, width_out):
    full = width_in // LANES
    blocks = [("a", i, j) for i in range(full) for j in range(i, full)]
    out_blocks = [
        ("g", i, j) for i in range(width_out // LANES) for j in range(i, width_out // LANES)
    ]
    cut = 2 * full - 1
    first = blocks[:cut] + out_blocks
    second = blocks[cut:]
    return first, second


def half_rows(width_in, width_out):
    first, second = layout(width_in, width_out)
    tail = width_in % LANES
    strips = -(-width_in // LANES)
    rows = max(len(first) * LANES, len(second) * LANES + strips * tail)
    return -(-rows // 64) * 64


def factor_kernel(where_ref, x_ref, g_ref, keep_ref, send_ref):
    width_in = x_ref.shape[1]
    width_out = g_ref.shape[2]
    full = width_in // LANES
    tail = width_in % LANES
    rows = keep_ref.shape[1]

    _, second = layout(width_in, width_out)
    strips = len(second) * LANES

    def panel(o_ref, tail_ref, i, start):
        lo = i * LANES
        hi = min(i + 2, full) * LANES
        sums = outer(x_ref[0, lo:, :], x_ref[0, lo:hi, :])
        at = start
        for b in range((hi - lo) // LANES):
            for j in range(b, full - i):
                o_ref[0, at : at + LANES, :] = sums[
                    j * LANES : (j + 1) * LANES, b * LANES : (b + 1) * LANES
                ]
                at += LANES
            if tail:
                row = strips + (i + b) * tail
                tail_ref[0, row : row + tail, :] = sums[
                    full * LANES - lo :, b * LANES : (b + 1) * LANES
                ]
        return at

    def halves(one_ref, two_ref):
        at = panel(one_ref, two_ref, 0, 0)
        sums = gram(g_ref[0], g_ref[0])
        for i in range(width_out // LANES):
            for j in range(i, width_out // LANES):
                one_ref[0, at : at + LANES, :] = sums[
                    j * LANES : (j + 1) * LANES, i * LANES : (i + 1) * LANES
                ]
                at += LANES
        if at < rows:
            one_ref[0, at:, :] = jnp.zeros((rows - at, LANES), F32)
        at = 0
        for i in range(2, full, 2):
            at = panel(two_ref, two_ref, i, at)
        at = strips
        if tail:
            last = x_ref[0, full * LANES :, :]
            at += full * tail
            two_ref[0, at : at + tail, :] = jnp.zeros((tail, LANES), F32)
            two_ref[0, at : at + tail, :tail] = outer(last, last)
            at += tail
        if at < rows:
            two_ref[0, at:, :] = jnp.zeros((rows - at, LANES), F32)

    @pl.when(where_ref[0] == 0)
    def _():
        halves(keep_ref, send_ref)

    @pl.when(where_ref[0] == 1)
    def _():
        halves(send_ref, keep_ref)


def factor_sums(where, first, layers, x, g):
    _, width_in, rows = x.shape
    width_out = g.shape[2]
    packed = half_rows(width_in, width_out)
    out = jax.ShapeDtypeStruct((layers, packed, LANES), F32)
    out_spec = pl.BlockSpec((1, packed, LANES), lambda l, s: (l, 0, 0))
    return pl.pallas_call(
        factor_kernel,
        out_shape=(out, out),
        grid_spec=pltpu.PrefetchScalarGridSpec(
            num_scalar_prefetch=1,
            grid=(layers,),
            in_specs=[
                pl.BlockSpec((1, width_in, rows), lambda l, s: ((l + first) ^ s[1], 0, 0)),
                pl.BlockSpec((1, rows, width_out), lambda l, s: ((l + first) ^ s[1], 0, 0)),
            ],
            out_specs=(out_spec, out_spec),
        ),
        compiler_params=pltpu.CompilerParams(vmem_limit_bytes=BIG_VMEM),
        cost_estimate=pl.CostEstimate(
            flops=layers * rows * width_in * width_in,
            bytes_accessed=layers * (rows * (width_in + width_out) * 2 + packed * LANES * 8),
            transcendentals=0,
        ),
        name="factor_sums",
    )(where, x, g)


def grad_kernel(core_ref, x_ref, g_ref, c_ref, keep_ref, send_ref):
    parts = [
        (g_ref[0, :, j : j + LANES].astype(F32) * c_ref[...]).astype(BF16)
        for j in range(0, g_ref.shape[2], LANES)
    ]
    sums = mm(x_ref[0], jnp.concatenate(parts, axis=1))

    @pl.when(core_ref[0] == 0)
    def _():
        keep_ref[0] = sums[:, :LANES]
        send_ref[0] = sums[:, LANES:]

    @pl.when(core_ref[0] == 1)
    def _():
        keep_ref[0] = sums[:, LANES:]
        send_ref[0] = sums[:, :LANES]


def grad_sums(where, x, g, centered):
    layers, width_in, rows = x.shape
    width_out = g.shape[2]
    out = jax.ShapeDtypeStruct((layers, width_in, LANES), F32)
    out_spec = pl.BlockSpec((1, width_in, LANES), lambda l, s: (l, 0, 0))
    return pl.pallas_call(
        grad_kernel,
        out_shape=(out, out),
        grid_spec=pltpu.PrefetchScalarGridSpec(
            num_scalar_prefetch=1,
            grid=(layers,),
            in_specs=[
                pl.BlockSpec((1, width_in, rows), lambda l, s: (l ^ s[1], 0, 0)),
                pl.BlockSpec((1, rows, width_out), lambda l, s: (l ^ s[1], 0, 0)),
                pl.BlockSpec((rows, LANES), lambda l, s: (0, 0)),
            ],
            out_specs=(out_spec, out_spec),
        ),
        compiler_params=pltpu.CompilerParams(vmem_limit_bytes=BIG_VMEM),
        cost_estimate=pl.CostEstimate(
            flops=2 * layers * rows * width_in * width_out,
            bytes_accessed=layers * (rows * (width_in + width_out) * 2 + width_in * width_out * 4),
            transcendentals=0,
        ),
        name="grad_sums",
    )(where, x, g, centered)


def split3(v):
    one = v.astype(BF16)
    rest = v - one.astype(F32)
    two = rest.astype(BF16)
    three = (rest - two.astype(F32)).astype(BF16)
    return one, two, three


def mm(a, b):
    return jnp.dot(a, b, preferred_element_type=F32)


def product(a, b):
    low = mm(a[0], b[2]) + mm(a[2], b[0]) + mm(a[1], b[1])
    return mm(a[0], b[0]) + (mm(a[0], b[1]) + mm(a[1], b[0]) + low)


def conjugate_gradients(apply, exact, b_ref, y_ref, r_ref, p_ref):
    def total(v):
        return jnp.sum(v, keepdims=True)

    def wanted(residual, size):
        return (residual - (TOL * DAMPING) ** 2 * size)[0, 0] > 0

    def body(state):
        step, residual, _ = state
        p = p_ref[...]
        q = apply(p)
        alpha = residual / total(p * q)
        y = y_ref[...] + alpha * p
        y_ref[...] = y
        r = r_ref[...] - alpha * q
        r_ref[...] = r
        fresh = total(r * r)
        p_ref[...] = r + (fresh / residual) * p
        return step + 1, fresh, wanted(fresh, total(y * y))

    def steps(start):
        r = r_ref[...]
        p_ref[...] = r
        residual = total(r * r)
        step, _, _ = lax.while_loop(
            lambda state: state[2] & (state[0] < MAX_STEPS),
            body,
            (start, residual, residual[0, 0] > 0),
        )
        return step

    y_ref[...] = jnp.zeros(y_ref.shape, F32)
    r_ref[...] = b_ref[...]
    if exact is None:
        steps(jnp.int32(0))
        return

    def cycle(state):
        step = steps(state[0])
        y = y_ref[...]
        r = b_ref[...] - exact(y)
        r_ref[...] = r
        return step, wanted(total(r * r), total(y * y))

    lax.while_loop(
        lambda state: state[1] & (state[0] < MAX_STEPS), cycle, (jnp.int32(0), jnp.bool_(True))
    )


def solve_kernel(
    all_rows,
    walkers,
    width_in,
    width_out,
    s_ref,
    own0,
    own1,
    own2,
    got0,
    got1,
    got2,
    mine_ref,
    other_ref,
    a0,
    a1,
    a2,
    g0,
    g1,
    g2,
    b_ref,
    t_ref,
    y_ref,
    r_ref,
    p_ref,
):
    full = width_in // LANES
    tail = width_in % LANES
    first, second = layout(width_in, width_out)
    terms = {"a": (a0, a1, a2), "g": (g0, g1, g2)}

    def put(kind, row, col, value):
        height, width = value.shape
        for ref, term in zip(terms[kind], split3(value)):
            ref[row : row + height, col : col + width] = term

    def place(kind, i, j, value):
        value = value * (1.0 / all_rows)
        if i == j:
            rows = lax.broadcasted_iota(jnp.int32, value.shape, 0)
            cols = lax.broadcasted_iota(jnp.int32, value.shape, 1)
            value = value + jnp.where(rows == cols, jnp.float32(DAMPING), 0.0)
        put(kind, j * LANES, i * LANES, value)
        if i != j:
            put(kind, i * LANES, j * LANES, value.T)

    def unpack(half, refs):
        rows = refs[0].shape[0]

        def read(at, height):
            return refs[at // rows][at % rows : at % rows + height, :]

        at = 0
        for kind, i, j in (first, second)[half]:
            place(kind, i, j, read(at, LANES))
            at += LANES
        if half == 1 and tail:
            edge = full * LANES
            for j in range(full):
                value = read(at, tail) * (1.0 / all_rows)
                put("a", edge, j * LANES, value)
                put("a", j * LANES, edge, jnp.concatenate([value, jnp.zeros_like(value)], 0).T[:, :tail])
                at += tail
            value = read(at, tail)[:, :tail] * (1.0 / all_rows)
            rows_at = lax.broadcasted_iota(jnp.int32, value.shape, 0)
            cols_at = lax.broadcasted_iota(jnp.int32, value.shape, 1)
            put("a", edge, edge, value + jnp.where(rows_at == cols_at, jnp.float32(DAMPING), 0.0))
        b_ref[:width_in, half * LANES : (half + 1) * LANES] = refs[2][...] * (2.0 / walkers)

    padded = a0.shape[0]
    if padded > width_in:
        for ref in terms["a"]:
            ref[width_in:, :] = jnp.zeros((padded - width_in, padded), BF16)
            ref[:, width_in:] = jnp.zeros((padded, padded - width_in), BF16)
        b_ref[width_in:, :] = jnp.zeros((padded - width_in, width_out), F32)
    core = s_ref[0]

    @pl.when(core == 0)
    def _():
        unpack(0, (own0, own1, own2))
        unpack(1, (got0, got1, got2))

    @pl.when(core == 1)
    def _():
        unpack(1, (own0, own1, own2))
        unpack(0, (got0, got1, got2))

    def near(p):
        one = p.astype(BF16)
        two = (p - one.astype(F32)).astype(BF16)
        return mm(a0[...], one) + (mm(a0[...], two) + mm(a1[...], one))

    conjugate_gradients(
        near,
        lambda p: product((a0[...], a1[...], a2[...]), split3(p)),
        b_ref,
        t_ref,
        r_ref,
        p_ref,
    )
    conjugate_gradients(
        lambda p: product(split3(p), (g0[...], g1[...], g2[...])), None, t_ref, y_ref, r_ref, p_ref
    )
    align = jnp.sum(y_ref[...] * b_ref[...])
    strip = mine_ref.shape[1] - 8

    def give(mine, other):
        for half in range(2):
            mine_ref[half, :strip, :] = mine[half * strip : (half + 1) * strip, :]
            mine_ref[half, strip:, :] = jnp.zeros((8, LANES), F32) + align
        other_ref[...] = other

    @pl.when(core == 0)
    def _():
        give(y_ref[:width_in, :LANES], y_ref[:width_in, LANES:])

    @pl.when(core == 1)
    def _():
        give(y_ref[:width_in, LANES:], y_ref[:width_in, :LANES])


def solve(scalars, own, got, all_rows, walkers, width_in, width_out):
    padded = -(-width_in // LANES) * LANES
    square = pltpu.VMEM((padded, padded), BF16)
    small = pltpu.VMEM((width_out, width_out), BF16)
    tall = pltpu.VMEM((padded, width_out), F32)
    return pl.pallas_call(
        functools.partial(solve_kernel, all_rows, walkers, width_in, width_out),
        out_shape=(
            jax.ShapeDtypeStruct((2, width_in // 2 + 8, LANES), F32),
            jax.ShapeDtypeStruct((width_in, LANES), F32),
        ),
        in_specs=[SMEM] + [VMEM] * 6,
        out_specs=(VMEM, VMEM),
        scratch_shapes=[square] * 3 + [small] * 3 + [tall] * 5,
        compiler_params=pltpu.CompilerParams(vmem_limit_bytes=BIG_VMEM),
        cost_estimate=pl.CostEstimate(
            flops=60 * width_in * width_in * width_out, bytes_accessed=4 << 20, transcendentals=0
        ),
        name="solve",
    )(scalars, *own, *got)


def finish_kernel(count, s_ref, mine, other, *refs):
    near, far, out_ref = refs[:6], refs[6:12], refs[12]
    core = s_ref[0]
    layer = s_ref[1]
    strip = mine.shape[1] - 8
    top = {0: mine[0], **{k: near[k - 1][...] for k in (1, 2, 3)}}
    low = {0: mine[1], **{k: near[k + 2][...] for k in (1, 2, 3)}}
    a = [top[k][strip : strip + 1, :] for k in range(4)]
    align = (a[0] + a[1]) + (a[2] + a[3])
    scale = jnp.sqrt(count / align)
    here = pl.ds(pl.multiple_of(core * LANES, LANES), LANES)
    there = pl.ds(pl.multiple_of((1 - core) * LANES, LANES), LANES)
    for k in range(4):
        at = layer ^ k
        out_ref[at, :strip, here] = top[k][:strip, :] * scale
        out_ref[at, strip:, here] = low[k][:strip, :] * scale
        if k:
            out_ref[at, :strip, there] = far[k - 1][:strip, :] * scale
            out_ref[at, strip:, there] = far[k + 2][:strip, :] * scale
        else:
            out_ref[at, :, there] = other[...] * scale


def finish(scalars, pieces, layers, width_in, width_out):
    return pl.pallas_call(
        functools.partial(finish_kernel, float(layers * width_in * width_out)),
        out_shape=jax.ShapeDtypeStruct((layers, width_in, width_out), F32),
        in_specs=[SMEM] + [VMEM] * len(pieces),
        out_specs=VMEM,
        compiler_params=pltpu.CompilerParams(vmem_limit_bytes=BIG_VMEM),
        name="finish",
    )(scalars, *pieces)


def swap(value, axis, bit):
    size = lax.axis_size(axis)
    return lax.ppermute(value, axis, [(i, i ^ bit) for i in range(size)])


def bit_of(axis, bit):
    return (lax.axis_index(axis) // bit) % 2


def pick(value, dim, index):
    return lax.dynamic_index_in_dim(value, index, dim, keepdims=False)


def shard_step(layer_inputs, layer_grads, local_energy):
    walk_count = lax.axis_size("walker")
    devices = walk_count * lax.axis_size("owner") * lax.axis_size("replica")
    per_walker = local_energy.shape[0]
    walkers = per_walker * devices
    layers, rows, width_in = layer_inputs.shape
    width_out = layer_grads.shape[2]
    all_rows = rows * devices

    core_bit = ("owner", 1)
    first_bit = ("walker", 1)
    second_bit = ("replica", 1)
    row_bits = [("owner", 2), ("replica", 2)]
    extra = 2
    while extra < walk_count:
        row_bits.append(("walker", extra))
        extra *= 2

    core = bit_of(*core_bit).astype(jnp.int32)
    bx = bit_of(*first_bit)
    bd = bit_of(*second_bit)
    layer = (2 * bx + bd).astype(jnp.int32)

    inputs = jnp.swapaxes(layer_inputs, 1, 2)
    scalars = jnp.stack([core, layer])
    tie = lax.optimization_barrier
    half = layers // 2

    total = jnp.broadcast_to(jnp.sum(local_energy), (8, LANES))

    def along(axes, value):
        size = 1
        for axis in axes:
            size *= lax.axis_size(axis)
        return [
            lax.ppermute(value, axes, [(i, (i + k) % size) for i in range(size)])
            for k in range(1, size)
        ]

    terms = along(("replica",), total)
    keep_far, send_far = factor_sums(scalars, half, half, inputs, layer_grads)
    keep_far, send_far, total, terms, where = tie((keep_far, send_far, total, terms, scalars))
    got_far = swap(send_far, *core_bit)
    total = total + sum(terms)
    terms = along(("owner",), total)
    where, total = tie((where, total))
    keep_own, send_own = factor_sums(where, 0, half, inputs, layer_grads)
    keep_own, send_own, total, terms, where = tie((keep_own, send_own, total, terms, where))
    got_own = swap(send_own, *core_bit)
    total = total + sum(terms)
    total = total + sum(along(("walker",), total))
    centered = local_energy[:, None] - total[:1, :] / walkers
    centered = jnp.repeat(centered, rows // per_walker, axis=0)

    bits = [first_bit, second_bit] + row_bits
    inner = (2,) * len(row_bits) + (-1, LANES)
    packed = keep_far.shape[1] // 2

    def start(parts, order):
        which = order[0]
        parts = [[v.reshape((2,) + inner) for v in pair] for pair in parts]
        if which == 0:
            return sum(parts[1]), sum(parts[0])
        if which == 1:
            return tuple(jnp.stack([sum(v[i] for v in pair) for pair in parts]) for i in (1, 0))
        mine = bit_of(*bits[which])
        return tuple(
            jnp.stack([sum(pick(v, which - 1, i) for v in pair) for pair in parts])
            for i in (1 - mine, mine)
        )

    rest = list(range(3, len(bits)))
    orders = [[0, 1, 2] + rest, [1, 0, 2] + rest, [2, 1, 0] + rest]
    out = keep_far[:, :packed] + got_far[:, :packed]
    out, where, centered = tie((out, where, centered))
    out_first = out.reshape((2,) + inner)
    keep_grads, send_grads = grad_sums(where, inputs, layer_grads, centered)
    got_grads = swap(send_grads, *core_bit)
    stay_first = (keep_own[:, :packed] + got_own[:, :packed]).reshape((2,) + inner)
    out_second, stay_second = start(
        [
            [keep_own[:, packed:], got_own[:, packed:]],
            [keep_far[:, packed:], got_far[:, packed:]],
        ],
        orders[1],
    )
    third = start(
        [[keep_grads[:half], got_grads[:half]], [keep_grads[half:], got_grads[half:]]], orders[2]
    )

    sums = []
    for colour, ((out, keep), order) in enumerate(
        zip([(out_first, stay_first), (out_second, stay_second), third], orders)
    ):
        got = swap(out, *bits[order[0]])
        left = list(range(len(bits)))
        left.remove(order[0])
        for which in order[1:]:
            dim = left.index(which)
            if which < 2:
                out = lax.index_in_dim(keep, 1, dim, False) + lax.index_in_dim(got, 1, dim, False)
                stay = lax.index_in_dim(keep, 0, dim, False) + lax.index_in_dim(got, 0, dim, False)
            else:
                mine = bit_of(*bits[which])
                out = pick(keep, dim, 1 - mine) + pick(got, dim, 1 - mine)
                stay = pick(keep, dim, mine) + pick(got, dim, mine)
            got = swap(out, *bits[which])
            keep = stay
            left.remove(which)
        piece = keep + got
        back = [w for w in order if w >= 2]
        if colour < 2:
            back = back[::-1]
        dims = []
        for which in back:
            mine = bit_of(*bits[which])
            other = swap(piece, *bits[which])
            index = lax.broadcasted_iota(jnp.int32, (2,) + piece.shape, 0)
            piece = jnp.where(index == mine, piece[None], other[None])
            dims.insert(0, which)
        rank = len(dims)
        axes = sorted(range(rank), key=lambda k: dims[k])
        piece = piece.transpose(*axes, rank, rank + 1).reshape(-1, LANES)
        sums.append(piece)

    got = [swap(piece, *core_bit) for piece in sums]
    mine, other = solve(scalars, sums, got, all_rows, walkers, width_in, width_out)

    top = {2: swap(mine[0], *first_bit), 1: swap(mine[0], *second_bit)}
    low = {1: swap(mine[1], *second_bit), 2: swap(mine[1], *first_bit)}
    top[3] = swap(top[2], *second_bit)
    low[3] = swap(low[1], *first_bit)
    near = [top[k] for k in (1, 2, 3)] + [low[k] for k in (1, 2, 3)]
    far = [swap(piece, *core_bit) for piece in near]
    return finish(scalars, (mine, other, *near, *far), layers, width_in, width_out)


def solution(mesh):
    in_specs = (
        P(None, ("walker", "owner", "replica"), None),
        P(None, ("walker", "owner", "replica"), None),
        P(("walker", "owner", "replica")),
    )
    return jax.shard_map(shard_step, mesh=mesh, in_specs=in_specs, out_specs=P(), check_vma=False)
```
